32 devices in a mesh: grp: 4 (over y, x), sub: 8 (over z, core).
Axes of the slice: x: 2, y: 2, z: 4, core: 2. Of those that a mesh axis runs over, the one named last changes fastest.
Arguments:
- reg_disp: float32 [4, 8, 3, 384], P('grp', 'sub'), may hold values from -6 to 6
- reg_vel: float32 [4, 8, 3, 384], P('grp', 'sub'), may hold values from -0.6 to 0.6
- site_disp: float32 [4, 8, 3, 1536], P('grp', 'sub'), may hold values from -6 to 6
- site_vel: float32 [4, 8, 3, 1536], P('grp', 'sub'), may hold values from -0.6 to 0.6
- reg_nodes: int32 [4, 8, 10, 256], P('grp', 'sub'), may hold values from 0 to 383
- site_nodes: int32 [4, 8, 35, 128], P('grp', 'sub'), may hold values from 0 to 1535
- reg_coefs: float32 [4, 8, 3, 3, 4, 256], P('grp', 'sub'), may hold values from -1.5 to 6, as said below
- site_coefs: float32 [4, 8, 3, 3, 24, 128], P('grp', 'sub'), may hold values from -1.5 to 6, as said below
- reg_table: float32 [12, 10], replicated, may hold values from -2 to 2
- site_table: float32 [72, 35], replicated, may hold values from -1 to 1
- reg_minv: float32 [4, 8, 384], P('grp', 'sub'), may hold values from 0.003 to 0.015
- site_minv: float32 [4, 8, 1536], P('grp', 'sub'), may hold values from 0.003 to 0.015
- reg_send: int32 [4, 8, 2, 128], P('grp', 'sub'), may hold values from 0 to 383
- reg_recv: int32 [4, 8, 2, 128], P('grp', 'sub'), may hold values from 0 to 383
- site_send: int32 [4, 8, 2, 128], P('grp', 'sub'), may hold values from 0 to 1535
- site_recv: int32 [4, 8, 2, 128], P('grp', 'sub'), may hold values from 0 to 1535
- slot_fill: int32 [4, 8, 4], P('grp', 'sub'), may hold values from 1 to 128, 384 in all within a row
- layer_src: int32 [4, 8, 128], P('grp', 'sub'), may hold values from 0 to 383
- layer_fill: int32 [4, 8], P('grp', 'sub'), may hold values from 64 to 128, as said below
- layer_dst: int32 [4, 8, 3, 128], P('grp', 'sub'), may hold values from 0 to 1535
- layer_stiff: float32 [4, 8, 3, 128], P('grp', 'sub'), may hold values from 0.5 to 2
Outputs:
- reg_final: float32 [4, 8, 3, 384], P('grp', 'sub')
- site_final: float32 [4, 8, 3, 1536], P('grp', 'sub')
The draws below stay inside these ranges and needn't reach their ends.
Inputs may be any that keep to these rules, and one draw needn't show every extreme that they name: `slot_fill`: per partition the four entries count live slots toward the lower and higher neighbour, regional then site; they sum to 384. `layer_fill`: partition index 0 of every group fills all 128 slots. `reg_coefs`: each 3 x 3 tensor over the first two dimensions is symmetric positive definite. `site_coefs`: each 3 x 3 tensor over the first two dimensions is symmetric positive definite.
All inputs are finite; a program needn't handle non-finite values.
Results may differ from the reference program's by a relative error of at most 0.0003.
Values sent between devices are 32-bit elements; how exact they have to be, the bound alone decides.
A program may use at most 64 MiB of HBM per device.

```python
import math
import jax
import jax.numpy as jnp
import numpy as np
from jax import lax

PR = 10
QR = 4
PS = 35
QS = 24
STEPS = 8
ES = 128
SLOTS = 128
DRM = 128
ER = 256
NR = 384
NS = 1536
N_GRP = 4
N_SUB = 8


def tensor_draw(key, quad_count, elem_count):
    first_key, second_key = jax.random.split(key)
    shape_diag = (N_GRP, N_SUB, 3, quad_count, elem_count)
    diagonal = jnp.exp(jax.random.uniform(first_key, shape_diag, jnp.float32, math.log(0.5), math.log(4.0)))
    off_diag = jax.random.uniform(second_key, (N_GRP, N_SUB, 3, 3, quad_count, elem_count), jnp.float32, -0.25, 0.25)
    off_diag = 0.5 * (off_diag + jnp.swapaxes(off_diag, 2, 3))
    identity = jnp.eye(3, dtype=jnp.float32)[:, :, None, None]
    off_diag = off_diag * (1.0 - identity)
    root_scale = jnp.sqrt(diagonal)
    return root_scale[:, :, :, None] * root_scale[:, :, None, :] * (identity + off_diag)


def draw_reg_coefs(key, part):
    return tensor_draw(jax.random.fold_in(key, 11), QR, ER)


def draw_site_coefs(key, part):
    return tensor_draw(jax.random.fold_in(key, 23), QS, ES)


def draw_layer_fill(key, part):
    counts = jax.random.randint(jax.random.fold_in(key, 37), (N_GRP, N_SUB), DRM // 2, DRM + 1, dtype=jnp.int32)
    return counts.at[:, 0].set(DRM)


def touch_ends(array, rng, low, high):
    place = [jax.random.randint(jax.random.fold_in(rng, axis), (), 0, length) for axis, length in enumerate(array.shape)]
    main_axis = array.shape.index(max(array.shape))
    next_to = place[:main_axis] + [(place[main_axis] + 1) % array.shape[main_axis]] + place[main_axis + 1:]
    return array.at[tuple(place)].set(low).at[tuple(next_to)].set(high)


def block_scale(key, shape, shards, low, high):
    def one(dim, blocks):
        heights = jax.random.uniform(jax.random.fold_in(jax.random.fold_in(key, 6), dim), (blocks,), jnp.float32, low / len(shards), high / len(shards))
        return jnp.repeat(jnp.exp(heights), shape[dim] // blocks).reshape((-1,) + (1,) * (len(shape) - dim - 1))

    loudness = one(*shards[0])
    for cut in shards[1:]:
        loudness = loudness * one(*cut)
    return loudness


def length_profile(count, total, bound, slope):
    weights = [(1 << 20) // math.isqrt(grade ** slope) + 1 for grade in range(2, count + 1)]
    surplus, given = total - bound - (count - 1), [1] * (count - 1)
    while surplus > 0:
        free = [i for i in range(count - 1) if given[i] < bound]
        whole, budget = sum([weights[i] for i in free]), surplus
        for i in free:
            more = min(bound - given[i], max(1, budget * weights[i] // whole), surplus)
            given[i] = given[i] + more
            surplus = surplus - more
    return np.array([bound] + given)


def ragged_sizes(stream_key, amount, total, limit, lean):
    if amount == 2:
        one = jax.random.randint(stream_key, (), max(1, total - limit), min(limit, total - 1) + 1)
        return jnp.stack([one, total - one])
    tallies = jnp.asarray(length_profile(amount, total, limit, lean), jnp.int32)
    couples = (amount - 1) // 2
    donor, sink = tallies[1:1 + 2 * couples:2], tallies[2:2 + 2 * couples:2]
    margin = jnp.minimum(donor - 1, limit - sink)
    passed = jax.random.randint(jax.random.fold_in(stream_key, 1), (couples,), 0, 1 << 20) % (margin + 1)
    tallies = tallies.at[1:1 + 2 * couples:2].set(donor - passed).at[2:2 + 2 * couples:2].set(sink + passed)
    return tallies[jax.random.permutation(jax.random.fold_in(stream_key, 2), amount)]


def scatter_about(rng, shape, spread, bound, shards=(), held_as=jnp.bfloat16):
    entries = jax.random.normal(rng, shape, jnp.float32) * spread
    if len(shards) > 0:
        entries = block_scale(rng, shape, shards, -0.22, 0.18) * entries
    return jnp.clip(entries, min=-bound, max=bound).astype(held_as)


def setup_inputs(seed: int = 0) -> dict:
    key_list = jax.random.split(jax.random.key(seed), 22)
    reg_disp = scatter_about(key_list[0], (N_GRP, N_SUB, 3, NR), 1.0, 6.0, ((0, 4), (1, 8)), jnp.float32)
    reg_vel = scatter_about(key_list[1], (N_GRP, N_SUB, 3, NR), 0.1, 0.6, ((0, 4), (1, 8)), jnp.float32)
    site_disp = scatter_about(key_list[2], (N_GRP, N_SUB, 3, NS), 1.0, 6.0, ((0, 4), (1, 8)), jnp.float32)
    site_vel = scatter_about(key_list[3], (N_GRP, N_SUB, 3, NS), 0.1, 0.6, ((0, 4), (1, 8)), jnp.float32)
    reg_nodes = touch_ends(jax.random.randint(key_list[4], (N_GRP, N_SUB, PR, ER), 0, NR), jax.random.fold_in(key_list[4], 1), 0, NR - 1).astype(jnp.int32)
    site_nodes = touch_ends(jax.random.randint(key_list[5], (N_GRP, N_SUB, PS, ES), 0, NS), jax.random.fold_in(key_list[5], 1), 0, NS - 1).astype(jnp.int32)
    reg_coefs = draw_reg_coefs(jax.random.fold_in(key_list[21], 71), 0)
    site_coefs = draw_site_coefs(jax.random.fold_in(key_list[21], 71), 0)
    reg_table = scatter_about(key_list[8], (3 * QR, PR), PR ** -0.5, 2.0, (), jnp.float32)
    site_table = scatter_about(key_list[9], (3 * QS, PS), PS ** -0.5, 1.0, (), jnp.float32)
    reg_minv = jnp.clip(jnp.exp(math.log(0.015) - 1.60943788 * jax.random.uniform(key_list[10], (N_GRP, N_SUB, NR), jnp.float32) ** block_scale(key_list[10], (N_GRP, N_SUB, NR), ((0, 4), (1, 8)), -0.2, 0.2)), 0.003, 0.015)
    site_minv = jnp.clip(jnp.exp(math.log(0.015) - 1.60943788 * jax.random.uniform(key_list[11], (N_GRP, N_SUB, NS), jnp.float32) ** block_scale(key_list[11], (N_GRP, N_SUB, NS), ((0, 4), (1, 8)), -0.2, 0.2)), 0.003, 0.015)
    reg_send = touch_ends(jax.random.randint(key_list[12], (N_GRP, N_SUB, 2, SLOTS), 0, NR), jax.random.fold_in(key_list[12], 1), 0, NR - 1).astype(jnp.int32)
    reg_recv = touch_ends(jax.random.randint(key_list[13], (N_GRP, N_SUB, 2, SLOTS), 0, NR), jax.random.fold_in(key_list[13], 1), 0, NR - 1).astype(jnp.int32)
    site_send = touch_ends(jax.random.randint(key_list[14], (N_GRP, N_SUB, 2, SLOTS), 0, NS), jax.random.fold_in(key_list[14], 1), 0, NS - 1).astype(jnp.int32)
    site_recv = touch_ends(jax.random.randint(key_list[15], (N_GRP, N_SUB, 2, SLOTS), 0, NS), jax.random.fold_in(key_list[15], 1), 0, NS - 1).astype(jnp.int32)
    slot_fill = jax.vmap(lambda own: ragged_sizes(own, 4, 3 * SLOTS, SLOTS, 0))(jax.random.split(key_list[16], N_GRP * N_SUB)).reshape((N_GRP, N_SUB, 4)).astype(jnp.int32)
    layer_src = touch_ends(jax.random.randint(key_list[17], (N_GRP, N_SUB, DRM), 0, NR), jax.random.fold_in(key_list[17], 1), 0, NR - 1).astype(jnp.int32)
    layer_fill = draw_layer_fill(jax.random.fold_in(key_list[21], 71), 0)
    layer_dst = touch_ends(jax.random.randint(key_list[19], (N_GRP, N_SUB, 3, DRM), 0, NS), jax.random.fold_in(key_list[19], 1), 0, NS - 1).astype(jnp.int32)
    layer_stiff = jnp.clip(jnp.exp(math.log(2.0) - 1.3862944 * jax.random.uniform(key_list[20], (N_GRP, N_SUB, 3, DRM), jnp.float32) ** block_scale(key_list[20], (N_GRP, N_SUB, 3, DRM), ((0, 4), (1, 8)), -0.2, 0.2)), 0.5, 2.0)
    return {"reg_disp": reg_disp, "reg_vel": reg_vel, "site_disp": site_disp, "site_vel": site_vel, "reg_nodes": reg_nodes, "site_nodes": site_nodes, "reg_coefs": reg_coefs, "site_coefs": site_coefs, "reg_table": reg_table, "site_table": site_table, "reg_minv": reg_minv, "site_minv": site_minv, "reg_send": reg_send, "reg_recv": reg_recv, "site_send": site_send, "site_recv": site_recv, "slot_fill": slot_fill, "layer_src": layer_src, "layer_fill": layer_fill, "layer_dst": layer_dst, "layer_stiff": layer_stiff}


PRECISE = lax.Precision.HIGHEST


def stiff_force(displaced, element_nodes, coef_block, deriv_table):
    quad_count = coef_block.shape[2]
    node_count = element_nodes.shape[0]
    elem_count = element_nodes.shape[1]
    flat_nodes = element_nodes.reshape(-1)
    gathered = jnp.take(displaced, flat_nodes, axis=1).reshape(3, node_count, elem_count)
    gradient = jnp.einsum("kp,cpe->cke", deriv_table, gathered, precision=PRECISE)
    pieces = [gradient[:, b * quad_count:(b + 1) * quad_count] for b in range(3)]
    flux_rows = [coef_block[a, 0][None] * pieces[0] + coef_block[a, 1][None] * pieces[1] + coef_block[a, 2][None] * pieces[2] for a in range(3)]
    flux_terms = jnp.concatenate(flux_rows, axis=1)
    element_terms = jnp.einsum("kp,cke->cpe", deriv_table, flux_terms, precision=PRECISE)
    return -jnp.zeros_like(displaced).at[:, flat_nodes].add(element_terms.reshape(3, -1))


def pack_slots(forces, send_map, fill_pair):
    picked = jnp.take(forces, send_map, axis=1)
    live_slots = jnp.arange(send_map.shape[1], dtype=jnp.int32)[None, :] < fill_pair[:, None]
    return jnp.where(live_slots[:, None, :], jnp.transpose(picked, (1, 0, 2)), 0.0)


def take_slots(forces, recv_map, from_lower, from_upper):
    return forces.at[:, recv_map[0]].add(from_lower).at[:, recv_map[1]].add(from_upper)


def pack_layer(displaced, layer_src, layer_fill):
    picked = jnp.take(displaced, layer_src, axis=1)
    live_slots = jnp.arange(layer_src.shape[0], dtype=jnp.int32) < layer_fill
    return jnp.where(live_slots[None, :], picked, 0.0)


def add_layer(forces, layer_dst, layer_stiff, layer_block):
    for source in range(3):
        forces = forces.at[:, layer_dst[source]].add(layer_stiff[source][None, :] * layer_block[source])
    return forces


def neighbour_terms(send_rows, group_rows):
    shaped = send_rows.reshape((group_rows, N_SUB) + send_rows.shape[1:])
    blank_rows = jnp.zeros_like(shaped[:, :1, 0])
    from_lower = jnp.concatenate([blank_rows, shaped[:, :-1, 1]], axis=1)
    from_upper = jnp.concatenate([shaped[:, 1:, 0], blank_rows], axis=1)
    width = send_rows.shape[-1]
    return from_lower.reshape(-1, 3, width), from_upper.reshape(-1, 3, width)


def reference(reg_disp, reg_vel, site_disp, site_vel, reg_nodes, site_nodes, reg_coefs, site_coefs, reg_table, site_table, reg_minv, site_minv, reg_send, reg_recv, site_send, site_recv, slot_fill, layer_src, layer_fill, layer_dst, layer_stiff):
    site_groups = N_GRP // 4
    reg_groups = 3 * site_groups

    def regional(stacked):
        return stacked[:reg_groups].reshape((reg_groups * N_SUB,) + stacked.shape[2:])

    def sitewise(stacked):
        return stacked[reg_groups:].reshape((site_groups * N_SUB,) + stacked.shape[2:])

    reg_now = regional(reg_disp)
    reg_prev = reg_now - regional(reg_vel)
    r_nodes, r_coefs, r_minv = regional(reg_nodes), regional(reg_coefs), regional(reg_minv)
    r_send, r_recv, r_fill = regional(reg_send), regional(reg_recv), regional(slot_fill)[:, 0:2]
    r_src, r_layer_fill = regional(layer_src), regional(layer_fill)
    layers = []
    for step_no in range(STEPS):
        forces = lax.map(lambda device_items: stiff_force(device_items[0], device_items[1], device_items[2], reg_table), (reg_now, r_nodes, r_coefs))
        send_rows = jax.vmap(pack_slots)(forces, r_send, r_fill)
        from_lower, from_upper = neighbour_terms(send_rows, reg_groups)
        forces = jax.vmap(take_slots)(forces, r_recv, from_lower, from_upper)
        reg_next = 2.0 * reg_now - reg_prev + r_minv[:, None, :] * forces
        reg_prev, reg_now = reg_now, reg_next
        layers.append(jax.vmap(pack_layer)(reg_now, r_src, r_layer_fill))

    site_now = sitewise(site_disp)
    site_prev = site_now - sitewise(site_vel)
    s_nodes, s_coefs, s_minv = sitewise(site_nodes), sitewise(site_coefs), sitewise(site_minv)
    s_send, s_recv, s_fill = sitewise(site_send), sitewise(site_recv), sitewise(slot_fill)[:, 2:4]
    s_dst, s_stiff = sitewise(layer_dst), sitewise(layer_stiff)
    for step_no in range(STEPS):
        forces = lax.map(lambda device_items: stiff_force(device_items[0], device_items[1], device_items[2], site_table), (site_now, s_nodes, s_coefs))
        send_rows = jax.vmap(pack_slots)(forces, s_send, s_fill)
        from_lower, from_upper = neighbour_terms(send_rows, site_groups)
        forces = jax.vmap(take_slots)(forces, s_recv, from_lower, from_upper)
        layer_block = layers[step_no].reshape(3, site_groups, N_SUB, 3, -1)
        layer_block = jnp.transpose(layer_block, (1, 2, 0, 3, 4)).reshape(site_groups * N_SUB, 3, 3, -1)
        forces = jax.vmap(add_layer)(forces, s_dst, s_stiff, layer_block)
        site_next = 2.0 * site_now - site_prev + s_minv[:, None, :] * forces
        site_prev, site_now = site_now, site_next

    reg_final = jnp.concatenate([reg_now.reshape((reg_groups, N_SUB) + reg_now.shape[1:]),
                                 jnp.zeros((site_groups, N_SUB) + reg_now.shape[1:], jnp.float32)], axis=0)
    site_final = jnp.concatenate([jnp.zeros((reg_groups, N_SUB) + site_now.shape[1:], jnp.float32),
                                  site_now.reshape((site_groups, N_SUB) + site_now.shape[1:])], axis=0)
    return reg_final, site_final
```

```python
import functools

import jax
import jax.numpy as jnp
from jax import lax
from jax.experimental import pallas as pl
from jax.experimental.pallas import tpu as pltpu
from jax.sharding import PartitionSpec as P

STEPS = 8
LANES = 128
MESH = pl.DeviceIdType.MESH
F32 = jnp.float32
BF16 = jnp.bfloat16


def up(size, unit):
    return -(-size // unit) * unit


def lane_gather(block, index):
    numbers = lax.GatherDimensionNumbers(
        offset_dims=(),
        collapsed_slice_dims=(1,),
        start_index_map=(1,),
        operand_batching_dims=(0,),
        start_indices_batching_dims=(0,),
    )
    return lax.gather(
        block,
        index[..., None],
        numbers,
        slice_sizes=(1, 1),
        mode=lax.GatherScatterMode.PROMISE_IN_BOUNDS,
    )


def split(value):
    high = value.astype(BF16)
    low = (value - high.astype(F32)).astype(BF16)
    return high, low


def dot(left, right):
    return jnp.dot(left, right, preferred_element_type=F32)


def spread(rows, blocks, row_block):
    lanes = rows[0].shape[1]
    mine = lax.broadcasted_iota(jnp.int32, (row_block, lanes), 0) == blocks
    return jnp.concatenate([jnp.where(mine, row, 0.0) for row in rows], axis=0).astype(BF16)


def spread_block(block, blocks, row_block):
    high = block.astype(BF16).astype(F32)
    low = block - high
    rows = [part[c : c + 1] for part in (high, low) for c in range(3)]
    return spread(rows, blocks, row_block)


def fill_onehot(out_ref, first_row, lanes_index, tmp_ref):
    count, length = lanes_index.shape
    tmp_ref[...] = jnp.zeros_like(tmp_ref)
    tmp_ref[0:count, :] = lanes_index.astype(F32)
    columns = tmp_ref[...].T
    lane = lax.broadcasted_iota(jnp.int32, (length, LANES), 1).astype(F32)
    for r in range(count):
        hot = jnp.where(lane == columns[:, r : r + 1], 1.0, 0.0)
        out_ref[first_row + r * length : first_row + (r + 1) * length, :] = hot.astype(BF16)


def pick(field, lanes_index, blocks, row_block):
    slots = lanes_index.shape[1]
    index = jnp.broadcast_to(lanes_index, (row_block, slots))
    mine = lax.broadcasted_iota(jnp.int32, (row_block, slots), 0) == blocks
    out = []
    for c in range(3):
        got = lane_gather(field[c * row_block : (c + 1) * row_block], index)
        out.append(jnp.sum(jnp.where(mine, got, 0.0), axis=0, keepdims=True))
    return out


def sizes(nodes_shape, coefs_shape, disp_shape):
    p, e = nodes_shape
    q = coefs_shape[-2]
    h = disp_shape[-1] // LANES
    qp = up(q, 8)
    return dict(p=p, e=e, q=q, h=h, hp=up(h, 8), qp=qp, p8=up(p, 8), pp=up(p, 16), kp=up(3 * qp, 16))


def role_scratch(d, extra_rows):
    return [
        pltpu.VMEM((d["p8"], d["e"]), jnp.int32),
        pltpu.VMEM((d["p8"], d["e"]), jnp.int32),
        pltpu.VMEM((d["p"] * d["e"], LANES), BF16),
        pltpu.VMEM((extra_rows * LANES, LANES), BF16),
        pltpu.VMEM((6 * d["hp"], d["p"] * d["e"]), BF16),
        pltpu.VMEM((2, d["pp"], 3 * d["e"]), F32),
        pltpu.VMEM((9, d["qp"], d["e"]), F32),
        pltpu.VMEM((2 * d["kp"], d["pp"]), BF16),
        pltpu.VMEM((2 * d["pp"], d["kp"]), BF16),
        pltpu.VMEM((3 * d["hp"], LANES), F32),
        pltpu.VMEM((3 * d["hp"], LANES), F32),
        pltpu.VMEM((3 * d["hp"], LANES), F32),
        pltpu.VMEM((LANES, d["e"]), F32),
    ]


def prepare(d, s, disp, vel, nodes, coefs, table, minv, slot_rows, square, tmp):
    (lane_ref, block_ref, hot_ref, slot_hot_ref, _, _, coef_ref, dd_ref, dt_ref, u_ref, prev_ref, minv_ref, tp) = s
    p, q, qp, kp, pp, hp = d["p"], d["q"], d["qp"], d["kp"], d["pp"], d["hp"]
    lane_ref[...] = jnp.zeros_like(lane_ref)
    block_ref[...] = jnp.full_like(block_ref, -1)
    lane_ref[0:p, :] = nodes[...] & (LANES - 1)
    block_ref[0:p, :] = nodes[...] >> 7
    fill_onehot(hot_ref, 0, nodes[...] & (LANES - 1), tp)
    row = 0
    for index in slot_rows:
        fill_onehot(slot_hot_ref, row, index & (LANES - 1), tmp)
        row += index.shape[0] * index.shape[1]
    if qp != q:
        coef_ref[...] = jnp.zeros_like(coef_ref)
    coef_ref[:, 0:q, :] = coefs[...]
    square[...] = jnp.zeros_like(square)
    for b in range(3):
        square[b * qp : b * qp + q, 0:p] = table[b * q : (b + 1) * q, :]
    high, low = split(square[0:kp, 0:pp])
    dd_ref[0:kp, :] = high
    dd_ref[kp : 2 * kp, :] = low
    turned = square[...].T
    square[...] = -turned
    high, low = split(square[0:pp, 0:kp])
    dt_ref[0:pp, :] = high
    dt_ref[pp : 2 * pp, :] = low
    for ref in (u_ref, prev_ref, minv_ref):
        ref[...] = jnp.zeros_like(ref)
    for c in range(3):
        for h in range(d["h"]):
            at, cut = c * hp + h, slice(h * LANES, (h + 1) * LANES)
            now = disp[c : c + 1, cut]
            u_ref[at : at + 1, :] = now
            prev_ref[at : at + 1, :] = now - vel[c : c + 1, cut]
            minv_ref[at : at + 1, :] = minv[0, :, cut]


def element_forces(d, s):
    (lane_ref, block_ref, hot_ref, _, left_ref, fe_ref, coef_ref, dd_ref, dt_ref, u_ref, _, _, _) = s
    p, e, qp, kp, pp, p8, hp = d["p"], d["e"], d["qp"], d["kp"], d["pp"], d["p8"], d["hp"]
    tiles = e // LANES
    got = [[jnp.zeros((p8, LANES), F32) for _ in range(tiles)] for _ in range(3)]
    for t in range(tiles):
        cut = slice(t * LANES, (t + 1) * LANES)
        lanes_index, blocks = lane_ref[:, cut], block_ref[:, cut]
        for h in range(d["h"]):
            mine = blocks == h
            for c in range(3):
                row = jnp.broadcast_to(u_ref[c * hp + h : c * hp + h + 1, :], (p8, LANES))
                got[c][t] = jnp.where(mine, lane_gather(row, lanes_index), got[c][t])
    nodal = jnp.concatenate([got[c][t] for c in range(3) for t in range(tiles)], axis=1)
    if pp != p8:
        nodal = jnp.concatenate([nodal, jnp.zeros((pp - p8, 3 * e), F32)], axis=0)
    high, low = split(nodal)
    both = dot(dd_ref[...], high)
    grad = both[0:kp] + both[kp:] + dot(dd_ref[0:kp, :], low)
    fluxes = []
    for c in range(3):
        cut = slice(c * e, (c + 1) * e)
        pieces = [grad[b * qp : (b + 1) * qp, cut] for b in range(3)]
        rows = [
            coef_ref[3 * a] * pieces[0] + coef_ref[3 * a + 1] * pieces[1] + coef_ref[3 * a + 2] * pieces[2]
            for a in range(3)
        ]
        if kp != 3 * qp:
            rows.append(jnp.zeros((kp - 3 * qp, e), F32))
        fluxes.append(jnp.concatenate(rows, axis=0))
    high, low = split(jnp.concatenate(fluxes, axis=1))
    both = dot(dt_ref[...], high)
    force = both[0:pp] + both[pp:] + dot(dt_ref[0:pp, :], low)
    high = force.astype(BF16).astype(F32)
    fe_ref[0] = high
    fe_ref[1] = force - high
    for n in range(p):
        rows = [fe_ref[k, n : n + 1, c * e : (c + 1) * e] for k in range(2) for c in range(3)]
        left_ref[:, n * e : (n + 1) * e] = spread(rows, block_ref[n : n + 1, :], hp)
    total = dot(left_ref[...], hot_ref[...])
    return total[0 : 3 * hp] + total[3 * hp :]


def kernel(
    n_grp, n_sub, rd, sd,
    reg_disp, reg_vel, site_disp, site_vel, reg_nodes, site_nodes, reg_coefs, site_coefs,
    reg_table, site_table, reg_minv, site_minv, reg_send, reg_recv, site_send, site_recv,
    slot_fill, layer_src, layer_fill, layer_dst, layer_stiff,
    reg_out, site_out,
    send_ref, recv_ref, layer_send_ref, layer_recv_ref, square, tmp,
    halo_send, halo_recv, layer_send, layer_recv,
    *scratch,
):
    half = len(scratch) // 2
    rs, ss = scratch[:half], scratch[half:]
    slots = reg_send.shape[1]
    sites = n_grp // 4
    regs = 3 * sites
    grp, sub = lax.axis_index("grp"), lax.axis_index("sub")
    is_site = grp >= regs
    has_low, has_high = sub > 0, sub < n_sub - 1
    source, part = grp // sites, grp % sites

    barrier = pltpu.get_barrier_semaphore()

    def greet(target):
        pl.semaphore_signal(barrier, inc=1, device_id=target, device_id_type=MESH)

    @pl.when(has_low)
    def _():
        greet((grp, sub - 1))

    @pl.when(has_high)
    def _():
        greet((grp, sub + 1))

    @pl.when(is_site)
    def _():
        for m in range(3):
            greet((m * sites + part, sub))

    def meet(others):
        peers = jnp.minimum(sub, 1) + jnp.minimum(n_sub - 1 - sub, 1) + others
        pl.semaphore_wait(barrier, peers)

    def halo(n, side):
        target = sub - 1 if side == 0 else sub + 1
        return pltpu.make_async_remote_copy(
            src_ref=send_ref.at[n, side],
            dst_ref=recv_ref.at[n, 1 - side],
            send_sem=halo_send.at[n, side],
            recv_sem=halo_recv.at[n, 1 - side],
            device_id=(grp, target),
            device_id_type=MESH,
        )

    def arrival(n, side):
        target = sub - 1 if side == 0 else sub + 1
        return pltpu.make_async_remote_copy(
            src_ref=send_ref.at[n, side],
            dst_ref=recv_ref.at[n, side],
            send_sem=halo_send.at[n, side],
            recv_sem=halo_recv.at[n, side],
            device_id=(grp, target),
            device_id_type=MESH,
        )

    def layer_copy(n, m):
        return pltpu.make_async_remote_copy(
            src_ref=layer_send_ref.at[n],
            dst_ref=layer_recv_ref.at[n, m],
            send_sem=layer_send.at[n],
            recv_sem=layer_recv.at[n, m],
            device_id=(regs + part, sub),
            device_id_type=MESH,
        )

    send_ref[...] = jnp.zeros_like(send_ref)

    @pl.when(jnp.logical_not(has_low))
    def _():
        recv_ref[:, 0] = jnp.zeros((STEPS, 8, slots), F32)

    @pl.when(jnp.logical_not(has_high))
    def _():
        recv_ref[:, 1] = jnp.zeros((STEPS, 8, slots), F32)

    lane = lax.broadcasted_iota(jnp.int32, (1, slots), 1)

    def exchange_start(n, force, send_map, first_fill, hp):
        for side in range(2):
            fill = slot_fill[0, :, first_fill + side : first_fill + side + 1]
            index = send_map[side : side + 1, :]
            blocks = jnp.where(lane < fill, index >> 7, -1)
            rows = pick(force, index & (LANES - 1), blocks, hp)
            for c in range(3):
                send_ref[n, side, c : c + 1, :] = rows[c]

        @pl.when(has_low)
        def _():
            halo(n, 0).start()

        @pl.when(has_high)
        def _():
            halo(n, 1).start()

    def exchange_end(n, recv_map, hot, hp):
        @pl.when(has_low)
        def _():
            arrival(n, 0).wait_recv()

        @pl.when(has_high)
        def _():
            arrival(n, 1).wait_recv()

        left = [
            spread_block(recv_ref[n, side], recv_map[side : side + 1, :] >> 7, hp) for side in range(2)
        ]
        total = dot(jnp.concatenate(left, axis=1), hot)
        return total[0 : 3 * hp] + total[3 * hp :]

    def step_on(s, force):
        u_ref, prev_ref, minv_ref = s[9], s[10], s[11]
        now = u_ref[...]
        later = 2.0 * now - prev_ref[...] + minv_ref[...] * force
        prev_ref[...] = now
        u_ref[...] = later
        return later

    def finish(d, s, out):
        for c in range(3):
            for h in range(d["h"]):
                at = c * d["hp"] + h
                out[c : c + 1, h * LANES : (h + 1) * LANES] = s[9][at : at + 1, :]

    def drain():
        def body(n, carry):
            @pl.when(has_low)
            def _():
                halo(n, 0).wait_send()

            @pl.when(has_high)
            def _():
                halo(n, 1).wait_send()

            return carry

        lax.fori_loop(0, STEPS, body, 0)

    @pl.when(jnp.logical_not(is_site))
    def _():
        site_out[...] = jnp.zeros_like(site_out)
        layer_send_ref[...] = jnp.zeros_like(layer_send_ref)
        prepare(rd, rs, reg_disp, reg_vel, reg_nodes, reg_coefs, reg_table, reg_minv, [reg_recv[...]], square, tmp)
        meet(1)
        hp = rd["hp"]

        def body(n, carry):
            force = element_forces(rd, rs)
            exchange_start(n, force, reg_send, 0, hp)
            force = force + exchange_end(n, reg_recv, rs[3][...], hp)
            later = step_on(rs, force)
            index = layer_src[0]
            blocks = jnp.where(lane < layer_fill[...], index >> 7, -1)
            rows = pick(later, index & (LANES - 1), blocks, hp)
            for c in range(3):
                layer_send_ref[n, c : c + 1, :] = rows[c]
            layer_copy(n, source).start()
            return carry

        lax.fori_loop(0, STEPS, body, 0)
        finish(rd, rs, reg_out)
        drain()

        def last(n, carry):
            layer_copy(n, source).wait_send()
            return carry

        lax.fori_loop(0, STEPS, last, 0)

    @pl.when(is_site)
    def _():
        reg_out[...] = jnp.zeros_like(reg_out)
        prepare(
            sd, ss, site_disp, site_vel, site_nodes, site_coefs, site_table, site_minv,
            [site_recv[...], layer_dst[...]], square, tmp,
        )
        meet(0)
        hp = sd["hp"]

        def body(n, carry):
            force = element_forces(sd, ss)
            exchange_start(n, force, site_send, 2, hp)
            for m in range(3):
                layer_copy(n, m).wait_recv()
            left = [
                spread_block(
                    layer_recv_ref[n, m] * layer_stiff[m : m + 1, :], layer_dst[m : m + 1, :] >> 7, hp
                )
                for m in range(3)
            ]
            total = dot(jnp.concatenate(left, axis=1), ss[3][2 * slots :, :])
            force = force + total[0 : 3 * hp] + total[3 * hp :]
            force = force + exchange_end(n, site_recv, ss[3][0 : 2 * slots, :], hp)
            step_on(ss, force)
            return carry

        lax.fori_loop(0, STEPS, body, 0)
        finish(sd, ss, site_out)
        drain()


def solution(mesh):
    n_grp, n_sub = mesh.shape["grp"], mesh.shape["sub"]

    def shards(*args):
        args = list(args)
        for k in (0, 1, 2, 3, 4, 5, 12, 13, 14, 15, 19, 20):
            args[k] = args[k].reshape(args[k].shape[2:])
        for k in (6, 7):
            args[k] = args[k].reshape((9,) + args[k].shape[4:])
        rd = sizes(args[4].shape, args[6].shape, args[0].shape)
        sd = sizes(args[5].shape, args[7].shape, args[2].shape)
        slots = args[12].shape[1]
        vmem = pl.BlockSpec(memory_space=pltpu.VMEM)
        reg_out, site_out = pl.pallas_call(
            functools.partial(kernel, n_grp, n_sub, rd, sd),
            out_shape=(
                jax.ShapeDtypeStruct(args[0].shape, F32),
                jax.ShapeDtypeStruct(args[2].shape, F32),
            ),
            in_specs=[vmem] * len(args),
            out_specs=(vmem, vmem),
            scratch_shapes=[
                pltpu.VMEM((STEPS, 2, 8, slots), F32),
                pltpu.VMEM((STEPS, 2, 8, slots), F32),
                pltpu.VMEM((STEPS, 8, slots), F32),
                pltpu.VMEM((STEPS, 3, 8, slots), F32),
                pltpu.VMEM((LANES, LANES), F32),
                pltpu.VMEM((LANES, slots), F32),
                pltpu.SemaphoreType.DMA((STEPS, 2)),
                pltpu.SemaphoreType.DMA((STEPS, 2)),
                pltpu.SemaphoreType.DMA((STEPS,)),
                pltpu.SemaphoreType.DMA((STEPS, 3)),
            ]
            + role_scratch(rd, 2)
            + role_scratch(sd, 5),
            compiler_params=pltpu.CompilerParams(
                collective_id=0, has_side_effects=True, vmem_limit_bytes=32 * 1024 * 1024
            ),
        )(*args)
        return reg_out[None, None], site_out[None, None]

    cell = ("grp", "sub")
    specs = [P(*cell)] * 21
    specs[8] = specs[9] = P()
    return jax.shard_map(
        shards,
        mesh=mesh,
        in_specs=tuple(specs),
        out_specs=(P(*cell), P(*cell)),
        check_vma=False,
    )
```

```python
import functools

import jax
import jax.numpy as jnp
from jax import lax
from jax.experimental import pallas as pl
from jax.experimental.pallas import tpu as pltpu
from jax.sharding import PartitionSpec as P

STEPS = 8
LANES = 128
MESH = pl.DeviceIdType.MESH
F32 = jnp.float32
BF16 = jnp.bfloat16


def up(size, unit):
    return -(-size // unit) * unit


def lane_gather(block, index):
    numbers = lax.GatherDimensionNumbers(
        offset_dims=(),
        collapsed_slice_dims=(1,),
        start_index_map=(1,),
        operand_batching_dims=(0,),
        start_indices_batching_dims=(0,),
    )
    return lax.gather(
        block,
        index[..., None],
        numbers,
        slice_sizes=(1, 1),
        mode=lax.GatherScatterMode.PROMISE_IN_BOUNDS,
    )


def split(value):
    high = value.astype(BF16)
    low = (value - high.astype(F32)).astype(BF16)
    return high, low


def dot(left, right):
    return jnp.dot(left, right, preferred_element_type=F32)


def spread(rows, blocks, row_block):
    lanes = rows[0].shape[1]
    mine = lax.broadcasted_iota(jnp.int32, (row_block, lanes), 0) == blocks
    return jnp.concatenate([jnp.where(mine, row, 0.0) for row in rows], axis=0).astype(BF16)


def spread_block(block, blocks, row_block):
    high = block.astype(BF16).astype(F32)
    low = block - high
    rows = [part[c : c + 1] for part in (high, low) for c in range(3)]
    return spread(rows, blocks, row_block)


def fill_onehot(out_ref, first_row, lanes_index, tmp_ref):
    count, length = len(lanes_index), lanes_index[0].shape[1]
    tmp_ref[...] = jnp.zeros_like(tmp_ref)
    for r, row in enumerate(lanes_index):
        tmp_ref[r : r + 1, :] = row.astype(F32)
    columns = tmp_ref[...].T
    lane = lax.broadcasted_iota(jnp.int32, (length, LANES), 1).astype(F32)
    for r in range(count):
        hot = jnp.where(lane == columns[:, r : r + 1], 1.0, 0.0)
        out_ref[first_row + r * length : first_row + (r + 1) * length, :] = hot.astype(BF16)


def pick(field, lanes_index, blocks, row_block):
    slots = lanes_index.shape[1]
    index = jnp.broadcast_to(lanes_index, (row_block, slots))
    mine = lax.broadcasted_iota(jnp.int32, (row_block, slots), 0) == blocks
    out = []
    for c in range(3):
        got = lane_gather(field[c * row_block : (c + 1) * row_block], index)
        out.append(jnp.sum(jnp.where(mine, got, 0.0), axis=0, keepdims=True))
    return out


def sizes(nodes_shape, coefs_shape, disp_shape):
    p, _, e = nodes_shape
    q = coefs_shape[-2]
    h = disp_shape[-1] // LANES
    qp = up(q, 8)
    return dict(p=p, e=e, q=q, h=h, hp=up(h, 8), qp=qp, p8=up(p, 8), pp=up(p, 16), kp=up(3 * qp, 16))


def role_scratch(d, extra_rows):
    return [
        pltpu.VMEM((d["p8"], d["e"]), jnp.int32),
        pltpu.VMEM((d["p8"], d["e"]), jnp.int32),
        pltpu.VMEM((d["p"] * d["e"], LANES), BF16),
        pltpu.VMEM((extra_rows * LANES, LANES), BF16),
        pltpu.VMEM((6 * d["hp"], d["p"] * d["e"]), BF16),
        pltpu.VMEM((2, d["pp"], 3 * d["e"]), F32),
        pltpu.VMEM((9, d["qp"], d["e"]), F32),
        pltpu.VMEM((2 * d["kp"], d["pp"]), BF16),
        pltpu.VMEM((2 * d["pp"], d["kp"]), BF16),
        pltpu.VMEM((3 * d["hp"], LANES), F32),
        pltpu.VMEM((3 * d["hp"], LANES), F32),
        pltpu.VMEM((3 * d["hp"], LANES), F32),
        pltpu.VMEM((LANES, d["e"]), F32),
    ]


def prepare(d, s, disp, vel, nodes, coefs, table, minv, slot_rows, square, tmp):
    (lane_ref, block_ref, hot_ref, slot_hot_ref, _, _, coef_ref, dd_ref, dt_ref, u_ref, prev_ref, minv_ref, tp) = s
    p, q, qp, kp, pp, hp = d["p"], d["q"], d["qp"], d["kp"], d["pp"], d["hp"]
    lane_ref[...] = jnp.zeros_like(lane_ref)
    block_ref[...] = jnp.full_like(block_ref, -1)
    for r in range(p):
        lane_ref[r : r + 1, :] = nodes[r] & (LANES - 1)
        block_ref[r : r + 1, :] = nodes[r] >> 7
    fill_onehot(hot_ref, 0, [nodes[r] & (LANES - 1) for r in range(p)], tp)
    fill_onehot(slot_hot_ref, 0, [row & (LANES - 1) for row in slot_rows], tmp)
    if qp != q:
        coef_ref[...] = jnp.zeros_like(coef_ref)
    coef_ref[:, 0:q, :] = coefs[...]
    square[...] = jnp.zeros_like(square)
    turned_table = table.shape[0] == p
    for b in range(3):
        if turned_table:
            square[0:p, b * qp : b * qp + q] = table[:, b * q : (b + 1) * q]
        else:
            square[b * qp : b * qp + q, 0:p] = table[b * q : (b + 1) * q, :]

    def plain():
        high, low = split(square[0:kp, 0:pp])
        dd_ref[0:kp, :] = high
        dd_ref[kp : 2 * kp, :] = low

    def turned():
        high, low = split(-square[0:pp, 0:kp])
        dt_ref[0:pp, :] = high
        dt_ref[pp : 2 * pp, :] = low

    first, second = (turned, plain) if turned_table else (plain, turned)
    first()
    square[...] = square[...].T
    second()
    for ref in (u_ref, prev_ref, minv_ref):
        ref[...] = jnp.zeros_like(ref)
    for c in range(3):
        for h in range(d["h"]):
            at, cut = c * hp + h, slice(h * LANES, (h + 1) * LANES)
            now = disp[c, :, cut]
            u_ref[at : at + 1, :] = now
            prev_ref[at : at + 1, :] = now - vel[c, :, cut]
            minv_ref[at : at + 1, :] = minv[0, :, cut]


def element_forces(d, s):
    (lane_ref, block_ref, hot_ref, _, left_ref, fe_ref, coef_ref, dd_ref, dt_ref, u_ref, _, _, _) = s
    p, e, qp, kp, pp, p8, hp = d["p"], d["e"], d["qp"], d["kp"], d["pp"], d["p8"], d["hp"]
    tiles = e // LANES
    got = [[jnp.zeros((p8, LANES), F32) for _ in range(tiles)] for _ in range(3)]
    for t in range(tiles):
        cut = slice(t * LANES, (t + 1) * LANES)
        lanes_index, blocks = lane_ref[:, cut], block_ref[:, cut]
        for h in range(d["h"]):
            mine = blocks == h
            for c in range(3):
                row = jnp.broadcast_to(u_ref[c * hp + h : c * hp + h + 1, :], (p8, LANES))
                got[c][t] = jnp.where(mine, lane_gather(row, lanes_index), got[c][t])
    nodal = jnp.concatenate([got[c][t] for c in range(3) for t in range(tiles)], axis=1)
    if pp != p8:
        nodal = jnp.concatenate([nodal, jnp.zeros((pp - p8, 3 * e), F32)], axis=0)
    high, low = split(nodal)
    both = dot(dd_ref[...], high)
    grad = both[0:kp] + both[kp:] + dot(dd_ref[0:kp, :], low)
    fluxes = []
    for c in range(3):
        cut = slice(c * e, (c + 1) * e)
        pieces = [grad[b * qp : (b + 1) * qp, cut] for b in range(3)]
        rows = [
            coef_ref[3 * a] * pieces[0] + coef_ref[3 * a + 1] * pieces[1] + coef_ref[3 * a + 2] * pieces[2]
            for a in range(3)
        ]
        if kp != 3 * qp:
            rows.append(jnp.zeros((kp - 3 * qp, e), F32))
        fluxes.append(jnp.concatenate(rows, axis=0))
    high, low = split(jnp.concatenate(fluxes, axis=1))
    both = dot(dt_ref[...], high)
    force = both[0:pp] + both[pp:] + dot(dt_ref[0:pp, :], low)
    high = force.astype(BF16).astype(F32)
    fe_ref[0] = high
    fe_ref[1] = force - high
    for n in range(p):
        rows = [fe_ref[k, n : n + 1, c * e : (c + 1) * e] for k in range(2) for c in range(3)]
        left_ref[:, n * e : (n + 1) * e] = spread(rows, block_ref[n : n + 1, :], hp)
    total = dot(left_ref[...], hot_ref[...])
    return total[0 : 3 * hp] + total[3 * hp :]


def kernel(
    n_grp, n_sub, rd, sd,
    reg_disp, reg_vel, site_disp, site_vel, reg_nodes, site_nodes, reg_coefs, site_coefs,
    reg_table, site_table, reg_minv, site_minv, reg_send, reg_recv, site_send, site_recv,
    slot_fill, layer_src, layer_fill, layer_dst, layer_stiff,
    reg_out, site_out,
    send_ref, recv_ref, layer_send_ref, layer_recv_ref, square, tmp,
    halo_send, halo_recv, layer_send, layer_recv,
    *scratch,
):
    half = len(scratch) // 2
    rs, ss = scratch[:half], scratch[half:]
    slots = reg_send.shape[1]
    sites = n_grp // 4
    regs = 3 * sites
    grp, sub = lax.axis_index("grp"), lax.axis_index("sub")
    is_site = grp >= regs
    has_low, has_high = sub > 0, sub < n_sub - 1
    source, part = grp // sites, grp % sites

    barrier = pltpu.get_barrier_semaphore()

    def greet(target):
        pl.semaphore_signal(barrier, inc=1, device_id=target, device_id_type=MESH)

    @pl.when(has_low)
    def _():
        greet((grp, sub - 1))

    @pl.when(has_high)
    def _():
        greet((grp, sub + 1))

    @pl.when(is_site)
    def _():
        for m in range(3):
            greet((m * sites + part, sub))

    def meet(others):
        peers = jnp.minimum(sub, 1) + jnp.minimum(n_sub - 1 - sub, 1) + others
        pl.semaphore_wait(barrier, peers)

    def halo(n, side):
        target = sub - 1 if side == 0 else sub + 1
        return pltpu.make_async_remote_copy(
            src_ref=send_ref.at[n, side],
            dst_ref=recv_ref.at[n, 1 - side],
            send_sem=halo_send.at[n, side],
            recv_sem=halo_recv.at[n, 1 - side],
            device_id=(grp, target),
            device_id_type=MESH,
        )

    def arrival(n, side):
        target = sub - 1 if side == 0 else sub + 1
        return pltpu.make_async_remote_copy(
            src_ref=send_ref.at[n, side],
            dst_ref=recv_ref.at[n, side],
            send_sem=halo_send.at[n, side],
            recv_sem=halo_recv.at[n, side],
            device_id=(grp, target),
            device_id_type=MESH,
        )

    def layer_copy(n, m):
        return pltpu.make_async_remote_copy(
            src_ref=layer_send_ref.at[n],
            dst_ref=layer_recv_ref.at[n, m],
            send_sem=layer_send.at[n],
            recv_sem=layer_recv.at[n, m],
            device_id=(regs + part, sub),
            device_id_type=MESH,
        )

    send_ref[...] = jnp.zeros_like(send_ref)

    @pl.when(jnp.logical_not(has_low))
    def _():
        recv_ref[:, 0] = jnp.zeros((STEPS, 8, slots), F32)

    @pl.when(jnp.logical_not(has_high))
    def _():
        recv_ref[:, 1] = jnp.zeros((STEPS, 8, slots), F32)

    lane = lax.broadcasted_iota(jnp.int32, (1, slots), 1)

    def exchange_start(n, force, send_map, first_fill, hp):
        for side in range(2):
            fill = slot_fill[0, :, first_fill + side : first_fill + side + 1]
            index = send_map[side : side + 1, :]
            blocks = jnp.where(lane < fill, index >> 7, -1)
            rows = pick(force, index & (LANES - 1), blocks, hp)
            for c in range(3):
                send_ref[n, side, c : c + 1, :] = rows[c]

        @pl.when(has_low)
        def _():
            halo(n, 0).start()

        @pl.when(has_high)
        def _():
            halo(n, 1).start()

    def exchange_end(n, recv_map, hot, hp):
        @pl.when(has_low)
        def _():
            arrival(n, 0).wait_recv()

        @pl.when(has_high)
        def _():
            arrival(n, 1).wait_recv()

        left = [
            spread_block(recv_ref[n, side], recv_map[side : side + 1, :] >> 7, hp) for side in range(2)
        ]
        total = dot(jnp.concatenate(left, axis=1), hot)
        return total[0 : 3 * hp] + total[3 * hp :]

    def step_on(s, force):
        u_ref, prev_ref, minv_ref = s[9], s[10], s[11]
        now = u_ref[...]
        later = 2.0 * now - prev_ref[...] + minv_ref[...] * force
        prev_ref[...] = now
        u_ref[...] = later
        return later

    def finish(d, s, out):
        for c in range(3):
            for h in range(d["h"]):
                at = c * d["hp"] + h
                out[c, :, h * LANES : (h + 1) * LANES] = s[9][at : at + 1, :]

    def drain():
        def body(n, carry):
            @pl.when(has_low)
            def _():
                halo(n, 0).wait_send()

            @pl.when(has_high)
            def _():
                halo(n, 1).wait_send()

            return carry

        lax.fori_loop(0, STEPS, body, 0)

    @pl.when(jnp.logical_not(is_site))
    def _():
        site_out[...] = jnp.zeros_like(site_out)
        layer_send_ref[...] = jnp.zeros_like(layer_send_ref)
        prepare(rd, rs, reg_disp, reg_vel, reg_nodes, reg_coefs, reg_table, reg_minv, [reg_recv[k : k + 1, :] for k in range(2)], square, tmp)
        meet(1)
        hp = rd["hp"]

        def body(n, carry):
            force = element_forces(rd, rs)
            exchange_start(n, force, reg_send, 0, hp)
            force = force + exchange_end(n, reg_recv, rs[3][...], hp)
            later = step_on(rs, force)
            index = layer_src[0]
            blocks = jnp.where(lane < layer_fill[...], index >> 7, -1)
            rows = pick(later, index & (LANES - 1), blocks, hp)
            for c in range(3):
                layer_send_ref[n, c : c + 1, :] = rows[c]
            layer_copy(n, source).start()
            return carry

        lax.fori_loop(0, STEPS, body, 0)
        finish(rd, rs, reg_out)
        drain()

        def last(n, carry):
            layer_copy(n, source).wait_send()
            return carry

        lax.fori_loop(0, STEPS, last, 0)

    @pl.when(is_site)
    def _():
        reg_out[...] = jnp.zeros_like(reg_out)
        prepare(
            sd, ss, site_disp, site_vel, site_nodes, site_coefs, site_table, site_minv,
            [site_recv[k : k + 1, :] for k in range(2)] + [layer_dst[m] for m in range(3)], square, tmp,
        )
        meet(0)
        hp = sd["hp"]

        def body(n, carry):
            force = element_forces(sd, ss)
            exchange_start(n, force, site_send, 2, hp)
            for m in range(3):
                layer_copy(n, m).wait_recv()
            left = [
                spread_block(
                    layer_recv_ref[n, m] * layer_stiff[m], layer_dst[m] >> 7, hp
                )
                for m in range(3)
            ]
            total = dot(jnp.concatenate(left, axis=1), ss[3][2 * slots :, :])
            force = force + total[0 : 3 * hp] + total[3 * hp :]
            force = force + exchange_end(n, site_recv, ss[3][0 : 2 * slots, :], hp)
            step_on(ss, force)
            return carry

        lax.fori_loop(0, STEPS, body, 0)
        finish(sd, ss, site_out)
        drain()


def solution(mesh):
    n_grp, n_sub = mesh.shape["grp"], mesh.shape["sub"]

    def shards(*args):
        args = list(args)
        for k in (0, 1, 2, 3, 4, 5, 19, 20):
            rows, length = args[k].shape[2:]
            args[k] = jnp.transpose(args[k], (0, 2, 1, 3)).reshape(rows, 1, length)
        for k in (12, 13, 14, 15):
            args[k] = args[k].reshape(args[k].shape[2:])
        args[9] = args[9].T
        for k in (6, 7):
            args[k] = args[k].reshape((9,) + args[k].shape[4:])
        rd = sizes(args[4].shape, args[6].shape, args[0].shape)
        sd = sizes(args[5].shape, args[7].shape, args[2].shape)
        slots = args[12].shape[1]
        vmem = pl.BlockSpec(memory_space=pltpu.VMEM)
        reg_out, site_out = pl.pallas_call(
            functools.partial(kernel, n_grp, n_sub, rd, sd),
            out_shape=(
                jax.ShapeDtypeStruct(args[0].shape, F32),
                jax.ShapeDtypeStruct(args[2].shape, F32),
            ),
            in_specs=[vmem] * len(args),
            out_specs=(vmem, vmem),
            scratch_shapes=[
                pltpu.VMEM((STEPS, 2, 8, slots), F32),
                pltpu.VMEM((STEPS, 2, 8, slots), F32),
                pltpu.VMEM((STEPS, 8, slots), F32),
                pltpu.VMEM((STEPS, 3, 8, slots), F32),
                pltpu.VMEM((LANES, LANES), F32),
                pltpu.VMEM((LANES, slots), F32),
                pltpu.SemaphoreType.DMA((STEPS, 2)),
                pltpu.SemaphoreType.DMA((STEPS, 2)),
                pltpu.SemaphoreType.DMA((STEPS,)),
                pltpu.SemaphoreType.DMA((STEPS, 3)),
            ]
            + role_scratch(rd, 2)
            + role_scratch(sd, 5),
            compiler_params=pltpu.CompilerParams(
                collective_id=0, has_side_effects=True
            ),
        )(*args)
        return tuple(out.reshape(1, 1, out.shape[0], out.shape[2]) for out in (reg_out, site_out))

    cell = ("grp", "sub")
    specs = [P(*cell)] * 21
    specs[8] = specs[9] = P()
    return jax.shard_map(
        shards,
        mesh=mesh,
        in_specs=tuple(specs),
        out_specs=(P(*cell), P(*cell)),
        check_vma=False,
    )
```
